256 devices in a mesh: groups: 4 (over x, y), row: 64 (over z, core).
Axes of the slice: x: 2, y: 2, z: 32, core: 2. Of those that a mesh axis runs over, the one named last changes fastest.
The devices are a block of a 4x8x32 slice.
Arguments:
- sub_vectors: float32 [32768, 2, 8192], P('groups', None, 'row'), parts along dimension 0, may hold values from -6 to 6
- eigen_values: float32 [2, 32768], P(None, ('groups', 'row')), parts along dimension 1, may hold values from -16384 to 16384, as said below
- kept: int32 [2, 32768], P(None, ('groups', 'row')), parts along dimension 1, may hold values from 0 to 1, as said below
- poles: int32 [2, 1024], P(None, 'groups'), parts along dimension 1, may hold values from 0 to 16383, as said below
- coupling: float32 [4], P('groups'), parts along dimension 0, may hold values from 0.5 to 2
Outputs:
- position: float32 [1024], P('groups'), parts along dimension 0
- merged: float32 [32768, 2, 256], P(('groups', 'row')), parts along dimension 0
The draws below stay inside these ranges and needn't reach their ends.
There are 4 independent parts, one for each index of `groups`. The reference program is written for one: setup_inputs(seed, part) draws one part's arguments, and reference() takes and returns one part's arrays. A program takes and returns all parts, laid end to end along the dimension named above; each array names one. Nothing has to cross between parts.
Inputs may be any that keep to these rules, and one draw needn't show every extreme that they name: `kept`: exactly 4096 entries are 0. All named entries are kept; poles[0, k] and poles[1, k] are neighbours among the kept eigenvalues in increasing order, poles[1, k] the larger; with S = 48, the rank of poles[0, k] among the kept eigenvalues (rank 0 the smallest) lies between k * S and (k + 1) * S - 2. `eigen_values`: all distinct; neighbouring values in sorted order differ by 0.25 or more.
All inputs are finite; a program needn't handle non-finite values.
Results may differ from the reference program's by a relative error of at most 0.0003.
Values sent between devices are 32-bit elements; how exact they have to be, the bound alone decides.
No kernel may reach another device: no remote copies, remote signals or barrier semaphores. Data moves between devices by JAX's collectives and lax.ppermute only.
A program may use at most 128 MiB of HBM per device.

```python
import math
import jax
import jax.numpy as jnp
from jax import lax

HALF = 8192
ORDER = 16384
ROOTS = 256
ITERS = 5


def structure(key):
    order = jax.random.permutation(jax.random.fold_in(key, 11), ORDER).astype(jnp.int32)
    dropped = jax.random.permutation(jax.random.fold_in(key, 12), ORDER)[:ORDER // 4]
    kept_sorted = jnp.ones((ORDER,), jnp.int32).at[dropped].set(0)
    kept_count = ORDER - ORDER // 4
    stride = kept_count // ROOTS
    sort_keys = jnp.where(kept_sorted == 1, 0, ORDER) + jnp.arange(ORDER, dtype=jnp.int32)
    kept_places = jnp.argsort(sort_keys)[:kept_count].astype(jnp.int32)
    jitter = jax.random.randint(jax.random.fold_in(key, 13), (ROOTS,), 0, stride - 1)
    ranks = (jnp.arange(ROOTS, dtype=jnp.int32) * stride + jitter).astype(jnp.int32)
    lower_place = kept_places[ranks]
    upper_place = kept_places[ranks + 1]
    kept_all = jnp.zeros((ORDER,), jnp.int32).at[order].set(kept_sorted)
    pole_index = jnp.stack([order[lower_place], order[upper_place]]).astype(jnp.int32)
    return (order, kept_all, pole_index)


def draw_eigen_values(key, part):
    order, kept_all, pole_index = structure(key)
    gap_key = jax.random.fold_in(key, 14)
    gaps = jax.random.uniform(gap_key, (ORDER,), jnp.float32, 0.5, 1.5)
    values = jnp.cumsum(gaps)
    values = values - 0.5 * values[-1]
    spread = jnp.zeros((ORDER,), jnp.float32).at[order].set(values)
    return spread.reshape(2, HALF)


def draw_kept(key, part):
    order, kept_all, pole_index = structure(key)
    return kept_all.reshape(2, HALF)


def draw_poles(key, part):
    order, kept_all, pole_index = structure(key)
    return pole_index


def block_levels(rng, dims, cuts, low, top_value):
    gain = 1.0
    for dim, shards_of in cuts:
        heights = jax.random.uniform(jax.random.fold_in(jax.random.fold_in(rng, 6), dim), (shards_of,), jnp.float32, low / len(cuts), top_value / len(cuts))
        gain = gain * jnp.repeat(jnp.exp(heights), dims[dim] // shards_of).reshape((-1,) + (1,) * (len(dims) - 1 - dim))
    return gain


def noise(rng, shape, width, limit, split=(), kind=jnp.bfloat16):
    array = jax.random.normal(rng, shape, jnp.float32) * width
    if len(split) > 0:
        array = block_levels(rng, shape, split, -0.22, 0.18) * array
    return jnp.clip(array, min=-limit, max=limit).astype(kind)


def setup_inputs(seed: int = 0, part: int = 0) -> dict:
    keys = jax.random.split(jax.random.key(seed), 6)
    part_splits = jax.random.split(jax.random.fold_in(keys[5], part), 6)
    sub_vectors = noise(part_splits[0], (HALF, 2, HALF), 1.0, 6.0, ((2, 64),), jnp.float32)
    eigen_values = draw_eigen_values(jax.random.fold_in(jax.random.fold_in(keys[5], part), 71), part)
    kept = draw_kept(jax.random.fold_in(jax.random.fold_in(keys[5], part), 71), part)
    poles = draw_poles(jax.random.fold_in(jax.random.fold_in(keys[5], part), 71), part)
    coupling = jnp.clip(jnp.exp(jax.random.uniform(part_splits[4], (1,), jnp.float32, math.log(0.5), math.log(2.0))), 0.5, 2.0)
    return {"sub_vectors": sub_vectors, "eigen_values": eigen_values, "kept": kept, "poles": poles, "coupling": coupling}


def secular_terms(weights, shifted, offset):
    inverse = 1.0 / (shifted - offset[:, None])
    part = weights[None, :] * inverse
    return (lax.optimization_barrier(jnp.sum(part, 1)), lax.optimization_barrier(jnp.sum(part * inverse, 1)))

def reference(sub_vectors, eigen_values, kept, poles, coupling):
    kept_float = kept.astype(jnp.float32)
    boundary = jnp.stack([sub_vectors[HALF - 1, 0, :], sub_vectors[0, 1, :]])
    masked_z = boundary * kept_float
    masked_d = eigen_values - 1000000.0 * (1.0 - kept_float)
    flat_d = masked_d.reshape(-1)
    pole_values = flat_d[poles]
    lower = pole_values[0]
    spacing = pole_values[1] - lower
    weights = (masked_z * masked_z).reshape(-1)
    shifted = flat_d[None, :] - lower[:, None]
    offset = 0.5 * spacing
    for step in range(ITERS):
        total, slope = secular_terms(weights, shifted, offset)
        moved = offset - (1.0 / coupling[0] + total) / slope
        offset = jnp.clip(moved, 0.02 * spacing, 0.98 * spacing)
    unused, norm_sq = secular_terms(weights, shifted, offset)
    position = offset / spacing
    normalizer = 1.0 / jnp.sqrt(norm_sq)
    vectors = masked_z[:, :, None] / (masked_d[:, :, None] - lower - offset) * normalizer
    merged = jnp.einsum('isj,sjk->isk', sub_vectors, vectors, precision=lax.Precision.HIGHEST)
    return (position, merged)
```

```python
import functools
import jax
import jax.numpy as jnp
from jax import lax
from jax.experimental import pallas as pl
from jax.experimental.pallas import tpu as pltpu
from jax.sharding import PartitionSpec as P

ITERS = 5
CORES = 2
SHARE = 4


VMEM = functools.partial(pl.BlockSpec, memory_space=pltpu.VMEM)
SMEM = functools.partial(pl.BlockSpec, memory_space=pltpu.SMEM)
ANY = functools.partial(pl.BlockSpec, memory_space=pl.ANY)


def params(mib):
    return pltpu.CompilerParams(vmem_limit_bytes=mib << 20)


def pack_kernel(last_ref, first_ref, value_ref, kept_ref, out_ref):
    kept = kept_ref[...].astype(jnp.float32)
    z0 = last_ref[6:7, :] * kept[0:1, :]
    z1 = first_ref[1:2, :] * kept[1:2, :]
    d = value_ref[...] - 1000000.0 * (1.0 - kept)
    four = jnp.concatenate([z0, z1, d], axis=0)
    out_ref[...] = jnp.broadcast_to(four[None], out_ref.shape)


def pack(flat, eigen_values, kept, chips):
    rows, cols = flat.shape
    return pl.pallas_call(
        pack_kernel,
        grid=(1,),
        in_specs=[
            pl.BlockSpec((8, cols), lambda i: (rows // 8 - 1, 0)),
            pl.BlockSpec((8, cols), lambda i: (0, 0)),
            pl.BlockSpec((2, cols), lambda i: (0, 0)),
            pl.BlockSpec((2, cols), lambda i: (0, 0)),
        ],
        out_specs=pl.BlockSpec((chips, 4, cols), lambda i: (0, 0, 0)),
        out_shape=jax.ShapeDtypeStruct((chips, 4, cols), jnp.float32),
        compiler_params=params(60),
        name="pack",
    )(flat, flat, eigen_values, kept)


def to_lanes(column):
    row = lax.broadcasted_iota(jnp.int32, column.shape, 0)
    lane = lax.broadcasted_iota(jnp.int32, column.shape, 1)
    return jnp.sum(jnp.where(row == lane, column, 0.0), axis=0, keepdims=True)


def secular_kernel(half, same_ref, other_ref, poles_ref, coupling_ref, roots_ref, bounds_ref, all_ref, d_ref, w_ref, pole_ref):
    me = lax.axis_index("row")
    core = lax.rem(me, CORES)
    slot = lax.rem(me, SHARE)
    count, cols = same_ref.shape
    all_ref[:count, :] = same_ref[...]
    all_ref[count:, :] = other_ref[...]
    blocks = count // 2
    for s in range(2):
        z = all_ref[pl.ds(s, blocks, stride=4), :]
        w_ref[s * blocks : (s + 1) * blocks, :] = z * z
        d_ref[s * blocks : (s + 1) * blocks, :] = all_ref[pl.ds(2 + s, blocks, stride=4), :]
    index = poles_ref[...]
    total = index.shape[0]
    s_of = index // half
    column = index - s_of * half
    device = column // cols
    lane_of = column - device * cols
    chip_of = device // CORES
    away = jnp.where(device - chip_of * CORES == core, 0, blocks // 2)
    row_of = s_of * blocks + away + chip_of
    rows = lax.broadcasted_iota(jnp.int32, (total, 2 * blocks), 1)
    pick = jnp.where(rows == row_of, 1.0, 0.0)
    picked = jnp.dot(pick, d_ref[...], precision=lax.Precision.HIGHEST, preferred_element_type=jnp.float32)
    lanes = lax.broadcasted_iota(jnp.int32, (total, cols), 1)
    value = jnp.sum(jnp.where(lanes == lane_of, picked, 0.0), axis=1, keepdims=True)
    pole_ref[...] = jnp.broadcast_to(value, (total, cols))
    roots = total // 2
    for t in range(roots // cols):
        low = to_lanes(pole_ref[t * cols : (t + 1) * cols, :])
        high = to_lanes(pole_ref[roots + t * cols : roots + (t + 1) * cols, :])
        bounds_ref[0:1, t * cols : (t + 1) * cols] = low
        bounds_ref[1:2, t * cols : (t + 1) * cols] = high - low
    own = roots // SHARE
    first = pl.multiple_of(slot * own, own)
    lower = pole_ref[pl.ds(first, own), :]
    spacing = pole_ref[pl.ds(roots + first, own), :] - lower
    inverse_coupling = 1.0 / jnp.full((own, cols), coupling_ref[0], jnp.float32)

    def sums(offset):
        def step(m, carry):
            total, slope = carry
            inverse = 1.0 / ((d_ref[pl.ds(m, 1), :] - lower) - offset)
            part = w_ref[pl.ds(m, 1), :] * inverse
            return total + part, slope + part * inverse

        zero = jnp.zeros((own, cols), jnp.float32)
        total, slope = lax.fori_loop(0, 2 * blocks, step, (zero, zero), unroll=4)
        spread = lambda a: jnp.broadcast_to(jnp.sum(a, axis=1, keepdims=True), (own, cols))
        return spread(total), spread(slope)

    def newton(_, offset):
        total, slope = sums(offset)
        moved = offset - (inverse_coupling + total) / slope
        return jnp.minimum(jnp.maximum(moved, 0.02 * spacing), 0.98 * spacing)

    offset = lax.fori_loop(0, ITERS, newton, 0.5 * spacing)
    _, norm_sq = sums(offset)
    row = lax.broadcasted_iota(jnp.int32, (own, cols), 0) + slot * own
    lane = lax.broadcasted_iota(jnp.int32, (own, cols), 1)
    for t in range(roots // cols):
        here = row == lane + t * cols
        for q, a in enumerate((offset, norm_sq)):
            roots_ref[q : q + 1, t * cols : (t + 1) * cols] = jnp.sum(jnp.where(here, a, 0.0), axis=0, keepdims=True)


def secular(same, other, poles, coupling, half):
    count, cols = same.shape
    roots = poles.shape[1]
    return pl.pallas_call(
        functools.partial(secular_kernel, half),
        in_specs=[VMEM(), VMEM(), VMEM(), SMEM()],
        out_specs=[VMEM(), VMEM()],
        out_shape=[jax.ShapeDtypeStruct((2, roots), jnp.float32)] * 2,
        scratch_shapes=[
            pltpu.VMEM((2 * count, cols), jnp.float32),
            pltpu.VMEM((count, cols), jnp.float32),
            pltpu.VMEM((count, cols), jnp.float32),
            pltpu.VMEM((2 * roots, cols), jnp.float32),
        ],
        compiler_params=params(8),
        cost_estimate=pl.CostEstimate(flops=20_000_000_000, bytes_accessed=400_000, transcendentals=0),
        name="secular",
    )(same, other, poles.reshape(-1, 1), coupling)


def vectors_kernel(same_ref, other_ref, a_ref, b_ref, c_ref, e_ref, bounds_ref, high_ref, low_ref, position_ref):
    me = lax.axis_index("row")
    chip = me // CORES
    cols = same_ref.shape[1]
    found = (a_ref[...] + b_ref[...]) + (c_ref[...] + e_ref[...])
    offset, norm_sq = found[0:1, :], found[1:2, :]
    lower, spacing = bounds_ref[0:1, :], bounds_ref[1:2, :]
    position_ref[...] = offset / spacing
    normalizer = 1.0 / jnp.sqrt(norm_sq)
    roots = offset.shape[1]
    for p, ref in enumerate((same_ref, other_ref)):
        for s in range(2):
            z = jnp.broadcast_to(ref[pl.ds(chip * 4 + s, 1), :], (cols, cols)).T
            d = jnp.broadcast_to(ref[pl.ds(chip * 4 + 2 + s, 1), :], (cols, cols)).T
            for t in range(roots // cols):
                k = slice(t * cols, (t + 1) * cols)
                v = z / ((d - lower[:, k]) - offset[:, k]) * normalizer[:, k]
                high = v.astype(jnp.bfloat16)
                high_ref[s, p * cols : (p + 1) * cols, k] = high
                low_ref[s, p * cols : (p + 1) * cols, k] = (v - high.astype(jnp.float32)).astype(jnp.bfloat16)


def make_vectors(same, other, found, bounds):
    cols = same.shape[1]
    roots = bounds.shape[1]
    return pl.pallas_call(
        vectors_kernel,
        in_specs=[VMEM()] * 7,
        out_specs=[VMEM()] * 3,
        out_shape=[
            jax.ShapeDtypeStruct((2, CORES * cols, roots), jnp.bfloat16),
            jax.ShapeDtypeStruct((2, CORES * cols, roots), jnp.bfloat16),
            jax.ShapeDtypeStruct((1, roots), jnp.float32),
        ],
        compiler_params=params(8),
        cost_estimate=pl.CostEstimate(flops=500_000_000, bytes_accessed=1_000_000, transcendentals=0),
        name="vectors",
    )(same, other, *found, bounds)


def product_kernel(distance, chips, own_ref, other_ref, high_ref, low_ref, *rest):
    *out_refs, own_buf, other_buf, sems = rest
    me = lax.axis_index("row")
    chip, core = me // CORES, lax.rem(me, CORES)
    chunk = lax.rem(chip + jnp.where(core == 0, distance, chips - distance), chips)
    count, length = own_buf.shape[:2]
    pairs = ((own_ref, own_buf), (other_ref, other_buf))

    def copy(h, q):
        start = chunk * (CORES * length) + lax.rem(core + h, 2) * length
        ref, buf = pairs[q]
        return pltpu.make_async_copy(ref.at[pl.ds(pl.multiple_of(start, length), length), :], buf.at[h], sems.at[h, q])

    for h in range(count):
        copy(h, 0).start()
        copy(h, 1).start()
    dot = functools.partial(jnp.dot, preferred_element_type=jnp.float32)

    for h in range(count):
        copy(h, 0).wait()
        copy(h, 1).wait()

        @pl.loop(0, 2)
        def _(s):
            a = own_buf[h, pl.ds(s, length // 2, stride=2), :]
            b = other_buf[h, pl.ds(s, length // 2, stride=2), :]
            x = jnp.concatenate([a, b], axis=1)
            high = x.astype(jnp.bfloat16)
            low = (x - high.astype(jnp.float32)).astype(jnp.bfloat16)
            out_refs[h][s] = (dot(low, high_ref[s]) + dot(high, low_ref[s])) + dot(high, high_ref[s])


def product(distance, count, chips, own, other, high, low):
    length = own.shape[0] // chips // CORES
    cols, roots = own.shape[1], high.shape[2]
    return pl.pallas_call(
        functools.partial(product_kernel, distance, chips),
        in_specs=[ANY(), ANY(), VMEM(), VMEM()],
        out_specs=[VMEM()] * count,
        out_shape=[jax.ShapeDtypeStruct((2, length // 2, roots), jnp.float32)] * count,
        scratch_shapes=[
            pltpu.VMEM((count, length, cols), jnp.float32),
            pltpu.VMEM((count, length, cols), jnp.float32),
            pltpu.SemaphoreType.DMA((count, 2)),
        ],
        compiler_params=params(8),
        cost_estimate=pl.CostEstimate(flops=count * 400_000_000, bytes_accessed=count * 800_000, transcendentals=0),
        name=f"product{distance}",
    )(own, other, high, low)


def finish_kernel(a_ref, b_ref, c_ref, out_ref):
    for s in range(2):
        out_ref[:, s, :] = (a_ref[s] + b_ref[s]) + c_ref[s]


def finish(a, b, c):
    _, rows, roots = a.shape
    return pl.pallas_call(
        finish_kernel,
        in_specs=[VMEM()] * 3,
        out_specs=VMEM(),
        out_shape=jax.ShapeDtypeStruct((rows, 2, roots), jnp.float32),
        compiler_params=params(8),
        name="finish",
    )(a, b, c)


def body(sub_vectors, eigen_values, kept, poles, coupling):
    rows, _, cols = sub_vectors.shape
    n = lax.axis_size("row")
    chips = n // CORES
    swap = [(i, i ^ 1) for i in range(n)]
    neighbour = [(i, i ^ CORES) for i in range(n)]
    diagonal = [(i, i ^ (CORES + 1)) for i in range(n)]
    onward = [(i, (i + CORES * (1 - 2 * (i % CORES))) % n) for i in range(n)]
    send = functools.partial(lax.ppermute, axis_name="row")

    own = sub_vectors.reshape(rows * 2, cols)
    other = send(own, perm=swap)
    packed = pack(own, eigen_values, kept, chips)
    groups = [[i for i in range(n) if i % CORES == c] for c in range(CORES)]
    same = lax.all_to_all(packed, "row", 0, 0, tiled=True, axis_index_groups=groups).reshape(chips * 4, cols)
    across = send(same, perm=swap)
    roots, bounds = secular(same, across, poles, coupling, n * cols)
    found = [roots] + [send(roots, perm=p) for p in (neighbour, diagonal, swap)]
    high, low, position = make_vectors(same, across, found, bounds)

    far = chips // 2
    first = product(far, 1, chips, own, other, high, low)
    streams = [send(first[0], perm=onward), None]
    for distance in range(far - 1, 0, -1):
        terms = product(distance, 2, chips, own, other, high, low)
        for h in range(2):
            total = terms[h] if streams[h] is None else streams[h] + terms[h]
            streams[h] = send(total, perm=onward)
    last = product(0, 1, chips, own, other, high, low)
    merged = finish(streams[0], last[0], send(streams[1], perm=swap))
    return (position.reshape(-1), merged)


def solution(mesh):
    in_specs = (
        P("groups", None, "row"),
        P(None, ("groups", "row")),
        P(None, ("groups", "row")),
        P(None, "groups"),
        P("groups"),
    )
    out_specs = (P("groups"), P(("groups", "row"), None, None))
    return jax.shard_map(body, mesh=mesh, in_specs=in_specs, out_specs=out_specs, check_vma=False)
```

```python
import functools
import jax
import jax.numpy as jnp
from jax import lax
from jax.experimental import pallas as pl
from jax.experimental.pallas import tpu as pltpu
from jax.sharding import PartitionSpec as P

ITERS = 5
CORES = 2
SHARE = 4


VMEM = functools.partial(pl.BlockSpec, memory_space=pltpu.VMEM)
SMEM = functools.partial(pl.BlockSpec, memory_space=pltpu.SMEM)
ANY = functools.partial(pl.BlockSpec, memory_space=pl.ANY)


def split_hops(chips):
    up = (chips - 1) // 2
    return up, chips - 1 - up


def params(mib):
    return pltpu.CompilerParams(vmem_limit_bytes=mib << 20)


def pack_kernel(last_ref, first_ref, value_ref, kept_ref, out_ref):
    kept = kept_ref[...].astype(jnp.float32)
    z0 = last_ref[6:7, :] * kept[0:1, :]
    z1 = first_ref[1:2, :] * kept[1:2, :]
    d = value_ref[...] - 1000000.0 * (1.0 - kept)
    four = jnp.concatenate([z0, z1, d], axis=0)
    out_ref[...] = jnp.broadcast_to(four[None], out_ref.shape)


def pack(flat, eigen_values, kept, chips):
    rows, cols = flat.shape
    return pl.pallas_call(
        pack_kernel,
        grid=(1,),
        in_specs=[
            pl.BlockSpec((8, cols), lambda i: (rows // 8 - 1, 0)),
            pl.BlockSpec((8, cols), lambda i: (0, 0)),
            pl.BlockSpec((2, cols), lambda i: (0, 0)),
            pl.BlockSpec((2, cols), lambda i: (0, 0)),
        ],
        out_specs=pl.BlockSpec((chips, 4, cols), lambda i: (0, 0, 0)),
        out_shape=jax.ShapeDtypeStruct((chips, 4, cols), jnp.float32),
        compiler_params=params(60),
        name="pack",
    )(flat, flat, eigen_values, kept)


def to_lanes(column):
    row = lax.broadcasted_iota(jnp.int32, column.shape, 0)
    lane = lax.broadcasted_iota(jnp.int32, column.shape, 1)
    return jnp.sum(jnp.where(row == lane, column, 0.0), axis=0, keepdims=True)


def secular_kernel(half, same_ref, other_ref, poles_ref, coupling_ref, roots_ref, bounds_ref, all_ref, d_ref, w_ref, pole_ref):
    me = lax.axis_index("row")
    core = lax.rem(me, CORES)
    slot = lax.rem(me, SHARE)
    count, cols = same_ref.shape
    all_ref[:count, :] = same_ref[...]
    all_ref[count:, :] = other_ref[...]
    blocks = count // 2
    for s in range(2):
        z = all_ref[pl.ds(s, blocks, stride=4), :]
        w_ref[s * blocks : (s + 1) * blocks, :] = z * z
        d_ref[s * blocks : (s + 1) * blocks, :] = all_ref[pl.ds(2 + s, blocks, stride=4), :]
    index = poles_ref[...]
    total = index.shape[0]
    s_of = index // half
    column = index - s_of * half
    device = column // cols
    lane_of = column - device * cols
    chip_of = device // CORES
    away = jnp.where(device - chip_of * CORES == core, 0, blocks // 2)
    row_of = s_of * blocks + away + chip_of
    rows = lax.broadcasted_iota(jnp.int32, (total, 2 * blocks), 1)
    pick = jnp.where(rows == row_of, 1.0, 0.0)
    picked = jnp.dot(pick, d_ref[...], precision=lax.Precision.HIGHEST, preferred_element_type=jnp.float32)
    lanes = lax.broadcasted_iota(jnp.int32, (total, cols), 1)
    value = jnp.sum(jnp.where(lanes == lane_of, picked, 0.0), axis=1, keepdims=True)
    pole_ref[...] = jnp.broadcast_to(value, (total, cols))
    roots = total // 2
    for t in range(roots // cols):
        low = to_lanes(pole_ref[t * cols : (t + 1) * cols, :])
        high = to_lanes(pole_ref[roots + t * cols : roots + (t + 1) * cols, :])
        bounds_ref[0:1, t * cols : (t + 1) * cols] = low
        bounds_ref[1:2, t * cols : (t + 1) * cols] = high - low
    own = roots // SHARE
    first = pl.multiple_of(slot * own, own)
    lower = pole_ref[pl.ds(first, own), :]
    spacing = pole_ref[pl.ds(roots + first, own), :] - lower
    inverse_coupling = 1.0 / jnp.full((own, cols), coupling_ref[0], jnp.float32)

    def sums(offset):
        def step(m, carry):
            total, slope = carry
            inverse = 1.0 / ((d_ref[pl.ds(m, 1), :] - lower) - offset)
            part = w_ref[pl.ds(m, 1), :] * inverse
            return total + part, slope + part * inverse

        zero = jnp.zeros((own, cols), jnp.float32)
        total, slope = lax.fori_loop(0, 2 * blocks, step, (zero, zero), unroll=4)
        spread = lambda a: jnp.broadcast_to(jnp.sum(a, axis=1, keepdims=True), (own, cols))
        return spread(total), spread(slope)

    def newton(_, offset):
        total, slope = sums(offset)
        moved = offset - (inverse_coupling + total) / slope
        return jnp.minimum(jnp.maximum(moved, 0.02 * spacing), 0.98 * spacing)

    offset = lax.fori_loop(0, ITERS, newton, 0.5 * spacing)
    _, norm_sq = sums(offset)
    row = lax.broadcasted_iota(jnp.int32, (own, cols), 0) + slot * own
    lane = lax.broadcasted_iota(jnp.int32, (own, cols), 1)
    for t in range(roots // cols):
        here = row == lane + t * cols
        for q, a in enumerate((offset, norm_sq)):
            roots_ref[q : q + 1, t * cols : (t + 1) * cols] = jnp.sum(jnp.where(here, a, 0.0), axis=0, keepdims=True)


def secular(same, other, poles, coupling, half):
    count, cols = same.shape
    roots = poles.shape[1]
    return pl.pallas_call(
        functools.partial(secular_kernel, half),
        in_specs=[VMEM(), VMEM(), VMEM(), SMEM()],
        out_specs=[VMEM(), VMEM()],
        out_shape=[jax.ShapeDtypeStruct((2, roots), jnp.float32)] * 2,
        scratch_shapes=[
            pltpu.VMEM((2 * count, cols), jnp.float32),
            pltpu.VMEM((count, cols), jnp.float32),
            pltpu.VMEM((count, cols), jnp.float32),
            pltpu.VMEM((2 * roots, cols), jnp.float32),
        ],
        compiler_params=params(8),
        cost_estimate=pl.CostEstimate(flops=20_000_000_000, bytes_accessed=400_000, transcendentals=0),
        name="secular",
    )(same, other, poles.reshape(-1, 1), coupling)


def vectors_kernel(same_ref, other_ref, a_ref, b_ref, c_ref, e_ref, bounds_ref, high_ref, low_ref, position_ref):
    me = lax.axis_index("row")
    chip = me // CORES
    cols = same_ref.shape[1]
    found = (a_ref[...] + b_ref[...]) + (c_ref[...] + e_ref[...])
    offset, norm_sq = found[0:1, :], found[1:2, :]
    lower, spacing = bounds_ref[0:1, :], bounds_ref[1:2, :]
    position_ref[...] = offset / spacing
    normalizer = 1.0 / jnp.sqrt(norm_sq)
    roots = offset.shape[1]
    for p, ref in enumerate((same_ref, other_ref)):
        for s in range(2):
            z = jnp.broadcast_to(ref[pl.ds(chip * 4 + s, 1), :], (cols, cols)).T
            d = jnp.broadcast_to(ref[pl.ds(chip * 4 + 2 + s, 1), :], (cols, cols)).T
            for t in range(roots // cols):
                k = slice(t * cols, (t + 1) * cols)
                v = z / ((d - lower[:, k]) - offset[:, k]) * normalizer[:, k]
                high = v.astype(jnp.bfloat16)
                high_ref[s, p * cols : (p + 1) * cols, k] = high
                low_ref[s, p * cols : (p + 1) * cols, k] = (v - high.astype(jnp.float32)).astype(jnp.bfloat16)


def make_vectors(same, other, found, bounds):
    cols = same.shape[1]
    roots = bounds.shape[1]
    return pl.pallas_call(
        vectors_kernel,
        in_specs=[VMEM()] * 7,
        out_specs=[VMEM()] * 3,
        out_shape=[
            jax.ShapeDtypeStruct((2, CORES * cols, roots), jnp.bfloat16),
            jax.ShapeDtypeStruct((2, CORES * cols, roots), jnp.bfloat16),
            jax.ShapeDtypeStruct((1, roots), jnp.float32),
        ],
        compiler_params=params(8),
        cost_estimate=pl.CostEstimate(flops=500_000_000, bytes_accessed=1_000_000, transcendentals=0),
        name="vectors",
    )(same, other, *found, bounds)


def product_kernel(chunks, chips, own_ref, other_ref, high_ref, low_ref, *rest):
    *out_refs, own_buf, other_buf, sems = rest
    me = lax.axis_index("row")
    chip, core = me // CORES, lax.rem(me, CORES)
    length = own_ref.shape[0] // chips // CORES
    used = jnp.logical_or(core != 0, chunks[-1][0] <= split_hops(chips)[0])

    @pl.when(used)
    def _():
        copies = []
        for n, (distance, count, _) in enumerate(chunks):
            chunk = lax.rem(chip + jnp.where(core == 0, distance, chips - distance), chips)
            copies.append([])
            for h in range(count):
                start = pl.multiple_of(chunk * (CORES * length) + lax.rem(core + h, 2) * length, length)
                for q, (ref, buf) in enumerate(((own_ref, own_buf), (other_ref, other_buf))):
                    copy = pltpu.make_async_copy(
                        ref.at[pl.ds(start, length), :], buf.at[n, pl.ds(h * length, length), :], sems.at[n, h, q]
                    )
                    copy.start()
                    copies[n].append(copy)
        dot = functools.partial(jnp.dot, preferred_element_type=jnp.float32)
        outs = iter(out_refs)
        for n, (_, count, pieces) in enumerate(chunks):
            refs = [next(outs) for _ in pieces]
            rows = count * length // 2
            for copy in copies[n]:
                copy.wait()

            @pl.loop(0, 2)
            def _(s):
                a = own_buf[n, pl.ds(s, rows, stride=2), :]
                b = other_buf[n, pl.ds(s, rows, stride=2), :]
                x = jnp.concatenate([a, b], axis=1)
                high = x.astype(jnp.bfloat16)
                low = (x - high.astype(jnp.float32)).astype(jnp.bfloat16)
                both = dot(jnp.concatenate([low, high], axis=0), high_ref[s])
                term = (both[:rows] + dot(high, low_ref[s])) + both[rows:]
                for ref, (first, last) in zip(refs, pieces):
                    ref[s] = term[first:last]


def product(chunks, chips, own, other, high, low):
    length = own.shape[0] // chips // CORES
    cols, roots = own.shape[1], high.shape[2]
    most = max(count for _, count, _ in chunks)
    work = sum(count for _, count, _ in chunks)
    pieces = [piece for _, _, some in chunks for piece in some]
    outs = pl.pallas_call(
        functools.partial(product_kernel, chunks, chips),
        in_specs=[ANY(), ANY(), VMEM(), VMEM()],
        out_specs=[VMEM()] * len(pieces),
        out_shape=[jax.ShapeDtypeStruct((2, last - first, roots), jnp.float32) for first, last in pieces],
        scratch_shapes=[
            pltpu.VMEM((len(chunks), most * length, cols), jnp.float32),
            pltpu.VMEM((len(chunks), most * length, cols), jnp.float32),
            pltpu.SemaphoreType.DMA((len(chunks), most, 2)),
        ],
        compiler_params=params(8),
        cost_estimate=pl.CostEstimate(flops=work * 300_000_000, bytes_accessed=work * 800_000, transcendentals=0),
        name=f"product{chunks[0][0]}",
    )(own, other, high, low)
    outs = iter(outs)
    return [[next(outs) for _ in some] for _, _, some in chunks]


def finish_kernel(first_ref, middle_ref, own_ref, near_ref, far_ref, out_ref):
    rows, head, tail = own_ref.shape[1], first_ref.shape[1], near_ref.shape[1]
    for start, stop in ((0, tail), (tail, head), (head, rows)):
        for s in range(2):
            here = first_ref[s, start:stop, :] if stop <= head else middle_ref[s, start - head : stop - head, :]
            there = near_ref[s, start:stop, :] if stop <= tail else far_ref[s, start - tail : stop - tail, :]
            out_ref[start:stop, s, :] = (here + own_ref[s, start:stop, :]) + there


def finish(first, middle, own, near, far):
    _, rows, roots = own.shape
    return pl.pallas_call(
        finish_kernel,
        in_specs=[VMEM()] * 5,
        out_specs=VMEM(),
        out_shape=jax.ShapeDtypeStruct((rows, 2, roots), jnp.float32),
        compiler_params=params(8),
        name="finish",
    )(first, middle, own, near, far)


def body(sub_vectors, eigen_values, kept, poles, coupling):
    rows, _, cols = sub_vectors.shape
    n = lax.axis_size("row")
    chips = n // CORES
    swap = [(i, i ^ 1) for i in range(n)]
    neighbour = [(i, i ^ CORES) for i in range(n)]
    diagonal = [(i, i ^ (CORES + 1)) for i in range(n)]
    onward = [(i, (i + CORES * (1 - 2 * (i % CORES))) % n) for i in range(n)]
    downward = [(i, j) for i, j in onward if i % CORES]
    send = functools.partial(lax.ppermute, axis_name="row")

    own = sub_vectors.reshape(rows * 2, cols)
    other = send(own, perm=swap)
    packed = pack(own, eigen_values, kept, chips)
    groups = [[i for i in range(n) if i % CORES == c] for c in range(CORES)]
    same = lax.all_to_all(packed, "row", 0, 0, tiled=True, axis_index_groups=groups).reshape(chips * 4, cols)
    across = send(same, perm=swap)
    roots, bounds = secular(same, across, poles, coupling, n * cols)
    found = [roots] + [send(roots, perm=p) for p in (neighbour, diagonal, swap)]
    high, low, position = make_vectors(same, across, found, bounds)

    half = rows // chips // CORES
    cut = -(-2 * half // 24) * 8
    pieces = ((0, cut), (cut, 2 * half - cut), (2 * half - cut, 2 * half))
    up, down = split_hops(chips)
    term = functools.partial(product, chips=chips, own=own, other=other, high=high, low=low)
    streams = None
    distance = down
    while distance > 0:
        span = 1 if distance == down or distance == 1 else 2
        chunks = [(d, 2, pieces) for d in range(distance, distance - span, -1)]
        for (d, _, _), terms in zip(chunks, term(chunks)):
            totals = terms if streams is None else [a + b for a, b in zip(streams, terms)]
            streams = [send(a, perm=onward if d <= up else downward) for a in totals]
        distance -= span
    ((last,),) = term([(0, 1, ((0, half),))])
    first, middle, other_rows = streams
    far_rows = send(other_rows, perm=swap)
    near_rows = send(middle[:, half - cut :, :], perm=swap)
    merged = finish(first, middle, last, near_rows, far_rows)
    return (position.reshape(-1), merged)


def solution(mesh):
    in_specs = (
        P("groups", None, "row"),
        P(None, ("groups", "row")),
        P(None, ("groups", "row")),
        P(None, "groups"),
        P("groups"),
    )
    out_specs = (P("groups"), P(("groups", "row"), None, None))
    return jax.shard_map(body, mesh=mesh, in_specs=in_specs, out_specs=out_specs, check_vma=False)
```

```python
import functools
import jax
import jax.numpy as jnp
from jax import lax
from jax.experimental import pallas as pl
from jax.experimental.pallas import tpu as pltpu
from jax.sharding import PartitionSpec as P

ITERS = 5
CORES = 2
SHARE = 4


VMEM = functools.partial(pl.BlockSpec, memory_space=pltpu.VMEM)
SMEM = functools.partial(pl.BlockSpec, memory_space=pltpu.SMEM)
ANY = functools.partial(pl.BlockSpec, memory_space=pl.ANY)


def role_of(chip, core):
    return (chip + core) % CORES


def params(mib):
    return pltpu.CompilerParams(vmem_limit_bytes=mib << 20)


def pack_kernel(last_ref, first_ref, value_ref, kept_ref, out_ref):
    kept = kept_ref[...].astype(jnp.float32)
    z0 = last_ref[6:7, :] * kept[0:1, :]
    z1 = first_ref[1:2, :] * kept[1:2, :]
    d = value_ref[...] - 1000000.0 * (1.0 - kept)
    four = jnp.concatenate([z0, z1, d], axis=0)
    out_ref[...] = jnp.broadcast_to(four[None], out_ref.shape)


def pack(flat, eigen_values, kept, chips):
    rows, cols = flat.shape
    return pl.pallas_call(
        pack_kernel,
        grid=(1,),
        in_specs=[
            pl.BlockSpec((8, cols), lambda i: (rows // 8 - 1, 0)),
            pl.BlockSpec((8, cols), lambda i: (0, 0)),
            pl.BlockSpec((2, cols), lambda i: (0, 0)),
            pl.BlockSpec((2, cols), lambda i: (0, 0)),
        ],
        out_specs=pl.BlockSpec((chips, 4, cols), lambda i: (0, 0, 0)),
        out_shape=jax.ShapeDtypeStruct((chips, 4, cols), jnp.float32),
        compiler_params=params(60),
        name="pack",
    )(flat, flat, eigen_values, kept)


def to_lanes(column):
    row = lax.broadcasted_iota(jnp.int32, column.shape, 0)
    lane = lax.broadcasted_iota(jnp.int32, column.shape, 1)
    return jnp.sum(jnp.where(row == lane, column, 0.0), axis=0, keepdims=True)


def secular_kernel(half, same_ref, other_ref, poles_ref, coupling_ref, roots_ref, bounds_ref, all_ref, d_ref, w_ref, pole_ref):
    me = lax.axis_index("row")
    core = lax.rem(me, CORES)
    slot = lax.rem(me, SHARE)
    count, cols = same_ref.shape
    all_ref[:count, :] = same_ref[...]
    all_ref[count:, :] = other_ref[...]
    blocks = count // 2
    for s in range(2):
        z = all_ref[pl.ds(s, blocks, stride=4), :]
        w_ref[s * blocks : (s + 1) * blocks, :] = z * z
        d_ref[s * blocks : (s + 1) * blocks, :] = all_ref[pl.ds(2 + s, blocks, stride=4), :]
    index = poles_ref[...]
    total = index.shape[0]
    s_of = index // half
    column = index - s_of * half
    device = column // cols
    lane_of = column - device * cols
    chip_of = device // CORES
    away = jnp.where(device - chip_of * CORES == core, 0, blocks // 2)
    row_of = s_of * blocks + away + chip_of
    rows = lax.broadcasted_iota(jnp.int32, (total, 2 * blocks), 1)
    pick = jnp.where(rows == row_of, 1.0, 0.0)
    picked = jnp.dot(pick, d_ref[...], precision=lax.Precision.HIGHEST, preferred_element_type=jnp.float32)
    lanes = lax.broadcasted_iota(jnp.int32, (total, cols), 1)
    value = jnp.sum(jnp.where(lanes == lane_of, picked, 0.0), axis=1, keepdims=True)
    pole_ref[...] = jnp.broadcast_to(value, (total, cols))
    roots = total // 2
    for t in range(roots // cols):
        low = to_lanes(pole_ref[t * cols : (t + 1) * cols, :])
        high = to_lanes(pole_ref[roots + t * cols : roots + (t + 1) * cols, :])
        bounds_ref[0:1, t * cols : (t + 1) * cols] = low
        bounds_ref[1:2, t * cols : (t + 1) * cols] = high - low
    own = roots // SHARE
    first = pl.multiple_of(slot * own, own)
    lower = pole_ref[pl.ds(first, own), :]
    spacing = pole_ref[pl.ds(roots + first, own), :] - lower
    inverse_coupling = 1.0 / jnp.full((own, cols), coupling_ref[0], jnp.float32)

    def sums(offset):
        def step(m, carry):
            total, slope = carry
            inverse = 1.0 / ((d_ref[pl.ds(m, 1), :] - lower) - offset)
            part = w_ref[pl.ds(m, 1), :] * inverse
            return total + part, slope + part * inverse

        zero = jnp.zeros((own, cols), jnp.float32)
        total, slope = lax.fori_loop(0, 2 * blocks, step, (zero, zero), unroll=4)
        spread = lambda a: jnp.broadcast_to(jnp.sum(a, axis=1, keepdims=True), (own, cols))
        return spread(total), spread(slope)

    def newton(_, offset):
        total, slope = sums(offset)
        moved = offset - (inverse_coupling + total) / slope
        return jnp.minimum(jnp.maximum(moved, 0.02 * spacing), 0.98 * spacing)

    offset = lax.fori_loop(0, ITERS, newton, 0.5 * spacing)
    _, norm_sq = sums(offset)
    row = lax.broadcasted_iota(jnp.int32, (own, cols), 0) + slot * own
    lane = lax.broadcasted_iota(jnp.int32, (own, cols), 1)
    for t in range(roots // cols):
        here = row == lane + t * cols
        for q, a in enumerate((offset, norm_sq)):
            roots_ref[q : q + 1, t * cols : (t + 1) * cols] = jnp.sum(jnp.where(here, a, 0.0), axis=0, keepdims=True)


def secular(same, other, poles, coupling, half):
    count, cols = same.shape
    roots = poles.shape[1]
    return pl.pallas_call(
        functools.partial(secular_kernel, half),
        in_specs=[VMEM(), VMEM(), VMEM(), SMEM()],
        out_specs=[VMEM(), VMEM()],
        out_shape=[jax.ShapeDtypeStruct((2, roots), jnp.float32)] * 2,
        scratch_shapes=[
            pltpu.VMEM((2 * count, cols), jnp.float32),
            pltpu.VMEM((count, cols), jnp.float32),
            pltpu.VMEM((count, cols), jnp.float32),
            pltpu.VMEM((2 * roots, cols), jnp.float32),
        ],
        compiler_params=params(8),
        cost_estimate=pl.CostEstimate(flops=20_000_000_000, bytes_accessed=400_000, transcendentals=0),
        name="secular",
    )(same, other, poles.reshape(-1, 1), coupling)


def vectors_kernel(same_ref, other_ref, a_ref, b_ref, c_ref, e_ref, bounds_ref, high_ref, low_ref, position_ref):
    me = lax.axis_index("row")
    chip = me // CORES
    cols = same_ref.shape[1]
    found = (a_ref[...] + b_ref[...]) + (c_ref[...] + e_ref[...])
    offset, norm_sq = found[0:1, :], found[1:2, :]
    lower, spacing = bounds_ref[0:1, :], bounds_ref[1:2, :]
    position_ref[...] = offset / spacing
    normalizer = 1.0 / jnp.sqrt(norm_sq)
    roots = offset.shape[1]
    for p, ref in enumerate((same_ref, other_ref)):
        for s in range(2):
            z = jnp.broadcast_to(ref[pl.ds(chip * 4 + s, 1), :], (cols, cols)).T
            d = jnp.broadcast_to(ref[pl.ds(chip * 4 + 2 + s, 1), :], (cols, cols)).T
            for t in range(roots // cols):
                k = slice(t * cols, (t + 1) * cols)
                v = z / ((d - lower[:, k]) - offset[:, k]) * normalizer[:, k]
                high = v.astype(jnp.bfloat16)
                high_ref[s, p * cols : (p + 1) * cols, k] = high
                low_ref[s, p * cols : (p + 1) * cols, k] = (v - high.astype(jnp.float32)).astype(jnp.bfloat16)


def make_vectors(same, other, found, bounds):
    cols = same.shape[1]
    roots = bounds.shape[1]
    return pl.pallas_call(
        vectors_kernel,
        in_specs=[VMEM()] * 7,
        out_specs=[VMEM()] * 3,
        out_shape=[
            jax.ShapeDtypeStruct((2, CORES * cols, roots), jnp.bfloat16),
            jax.ShapeDtypeStruct((2, CORES * cols, roots), jnp.bfloat16),
            jax.ShapeDtypeStruct((1, roots), jnp.float32),
        ],
        compiler_params=params(8),
        cost_estimate=pl.CostEstimate(flops=500_000_000, bytes_accessed=1_000_000, transcendentals=0),
        name="vectors",
    )(same, other, *found, bounds)


def product_kernel(chunks, chips, own_ref, other_ref, high_ref, low_ref, *rest):
    *out_refs, own_buf, other_buf, sems = rest
    me = lax.axis_index("row")
    chip, core = me // CORES, lax.rem(me, CORES)
    length = own_ref.shape[0] // chips // CORES
    role = lax.rem(chip + core, CORES)
    copies = []
    for n, (distance, count, _) in enumerate(chunks):
        chunk = lax.rem(chip + jnp.where(role == 0, distance, chips - distance), chips)
        copies.append([])
        for h in range(count):
            start = pl.multiple_of(chunk * (CORES * length) + lax.rem(role + chunk + h, 2) * length, length)
            for q, (ref, buf) in enumerate(((own_ref, own_buf), (other_ref, other_buf))):
                copy = pltpu.make_async_copy(
                    ref.at[pl.ds(start, length), :], buf.at[n, pl.ds(h * length, length), :], sems.at[n, h, q]
                )
                copy.start()
                copies[n].append(copy)
    dot = functools.partial(jnp.dot, preferred_element_type=jnp.float32)
    outs = iter(out_refs)
    for n, (_, count, pieces) in enumerate(chunks):
        refs = [next(outs) for _ in pieces]
        rows = count * length // 2
        for copy in copies[n]:
            copy.wait()

        @pl.loop(0, 2)
        def _(s):
            a = own_buf[n, pl.ds(s, rows, stride=2), :]
            b = other_buf[n, pl.ds(s, rows, stride=2), :]
            x = jnp.concatenate([a, b], axis=1)
            high = x.astype(jnp.bfloat16)
            low = (x - high.astype(jnp.float32)).astype(jnp.bfloat16)
            both = dot(jnp.concatenate([low, high], axis=0), high_ref[s])
            term = (both[:rows] + dot(high, low_ref[s])) + both[rows:]
            for ref, (first, last) in zip(refs, pieces):
                ref[s] = term[first:last]


def product(chunks, chips, own, other, high, low):
    length = own.shape[0] // chips // CORES
    cols, roots = own.shape[1], high.shape[2]
    most = max(count for _, count, _ in chunks)
    work = sum(count for _, count, _ in chunks)
    pieces = [piece for _, _, some in chunks for piece in some]
    outs = pl.pallas_call(
        functools.partial(product_kernel, chunks, chips),
        in_specs=[ANY(), ANY(), VMEM(), VMEM()],
        out_specs=[VMEM()] * len(pieces),
        out_shape=[jax.ShapeDtypeStruct((2, last - first, roots), jnp.float32) for first, last in pieces],
        scratch_shapes=[
            pltpu.VMEM((len(chunks), most * length, cols), jnp.float32),
            pltpu.VMEM((len(chunks), most * length, cols), jnp.float32),
            pltpu.SemaphoreType.DMA((len(chunks), most, 2)),
        ],
        compiler_params=params(8),
        cost_estimate=pl.CostEstimate(flops=work * 300_000_000, bytes_accessed=work * 800_000, transcendentals=0),
        name=f"product{chunks[0][0]}",
    )(own, other, high, low)
    outs = iter(outs)
    return [[next(outs) for _ in some] for _, _, some in chunks]


def finish_kernel(a_ref, b_ref, c_ref, out_ref):
    for s in range(2):
        out_ref[:, s, :] = (a_ref[s] + b_ref[s]) + c_ref[s]


def finish(a, b, c):
    _, rows, roots = a.shape
    return pl.pallas_call(
        finish_kernel,
        in_specs=[VMEM()] * 3,
        out_specs=VMEM(),
        out_shape=jax.ShapeDtypeStruct((rows, 2, roots), jnp.float32),
        compiler_params=params(8),
        name="finish",
    )(a, b, c)


def body(sub_vectors, eigen_values, kept, poles, coupling):
    rows, _, cols = sub_vectors.shape
    n = lax.axis_size("row")
    chips = n // CORES
    swap = [(i, i ^ 1) for i in range(n)]
    neighbour = [(i, i ^ CORES) for i in range(n)]
    diagonal = [(i, i ^ (CORES + 1)) for i in range(n)]
    onward = []
    for i in range(n):
        chip, core = i // CORES, i % CORES
        there = (chip + (1, -1)[role_of(chip, core)]) % chips
        onward.append((i, there * CORES + (1 - core)))
    send = functools.partial(lax.ppermute, axis_name="row")

    own = sub_vectors.reshape(rows * 2, cols)
    other = send(own, perm=swap)
    packed = pack(own, eigen_values, kept, chips)
    groups = [[i for i in range(n) if i % CORES == c] for c in range(CORES)]
    same = lax.all_to_all(packed, "row", 0, 0, tiled=True, axis_index_groups=groups).reshape(chips * 4, cols)
    across = send(same, perm=swap)
    roots, bounds = secular(same, across, poles, coupling, n * cols)
    found = [roots] + [send(roots, perm=p) for p in (neighbour, diagonal, swap)]
    high, low, position = make_vectors(same, across, found, bounds)

    half = rows // chips // CORES
    both = ((0, half), (half, 2 * half))
    far = chips // 2
    term = functools.partial(product, chips=chips, own=own, other=other, high=high, low=low)
    (first,) = term([(far, 1, both[:1])])
    streams = [send(first[0], perm=onward), None]
    distance = far - 1
    while distance > 0:
        span = 1 if distance == far - 1 or distance == 1 else 2
        for terms in term([(d, 2, both) for d in range(distance, distance - span, -1)]):
            totals = [b if a is None else a + b for a, b in zip(streams, terms)]
            streams = [send(a, perm=onward) for a in totals]
        distance -= span
    ((last,),) = term([(0, 1, both[:1])])
    merged = finish(streams[0], last, send(streams[1], perm=swap))
    return (position.reshape(-1), merged)


def solution(mesh):
    in_specs = (
        P("groups", None, "row"),
        P(None, ("groups", "row")),
        P(None, ("groups", "row")),
        P(None, "groups"),
        P("groups"),
    )
    out_specs = (P("groups"), P(("groups", "row"), None, None))
    return jax.shard_map(body, mesh=mesh, in_specs=in_specs, out_specs=out_specs, check_vma=False)
```

```python
import functools
import jax
import jax.numpy as jnp
from jax import lax
from jax.experimental import pallas as pl
from jax.experimental.pallas import tpu as pltpu
from jax.sharding import PartitionSpec as P

ITERS = 5
CORES = 2
SHARE = 4


VMEM = functools.partial(pl.BlockSpec, memory_space=pltpu.VMEM)
SMEM = functools.partial(pl.BlockSpec, memory_space=pltpu.SMEM)
ANY = functools.partial(pl.BlockSpec, memory_space=pl.ANY)


def role_of(chip, core):
    return (chip + core) % CORES


def params(mib):
    return pltpu.CompilerParams(vmem_limit_bytes=mib << 20)


def pack_kernel(last_ref, first_ref, value_ref, kept_ref, out_ref):
    kept = kept_ref[...].astype(jnp.float32)
    z0 = last_ref[6:7, :] * kept[0:1, :]
    z1 = first_ref[1:2, :] * kept[1:2, :]
    d = value_ref[...] - 1000000.0 * (1.0 - kept)
    four = jnp.concatenate([z0, z1, d], axis=0)
    out_ref[...] = jnp.broadcast_to(four[None], out_ref.shape)


def pack(flat, eigen_values, kept, chips):
    rows, cols = flat.shape
    return pl.pallas_call(
        pack_kernel,
        grid=(1,),
        in_specs=[
            pl.BlockSpec((8, cols), lambda i: (rows // 8 - 1, 0)),
            pl.BlockSpec((8, cols), lambda i: (0, 0)),
            pl.BlockSpec((2, cols), lambda i: (0, 0)),
            pl.BlockSpec((2, cols), lambda i: (0, 0)),
        ],
        out_specs=pl.BlockSpec((chips, 4, cols), lambda i: (0, 0, 0)),
        out_shape=jax.ShapeDtypeStruct((chips, 4, cols), jnp.float32),
        compiler_params=params(60),
        name="pack",
    )(flat, flat, eigen_values, kept)


def to_lanes(column):
    row = lax.broadcasted_iota(jnp.int32, column.shape, 0)
    lane = lax.broadcasted_iota(jnp.int32, column.shape, 1)
    return jnp.sum(jnp.where(row == lane, column, 0.0), axis=0, keepdims=True)


def secular_kernel(half, same_ref, other_ref, poles_ref, coupling_ref, roots_ref, bounds_ref, all_ref, d_ref, w_ref, pole_ref):
    me = lax.axis_index("row")
    core = lax.rem(me, CORES)
    slot = lax.rem(me, SHARE)
    count, cols = same_ref.shape
    all_ref[:count, :] = same_ref[...]
    all_ref[count:, :] = other_ref[...]
    blocks = count // 2
    for s in range(2):
        z = all_ref[pl.ds(s, blocks, stride=4), :]
        w_ref[s * blocks : (s + 1) * blocks, :] = z * z
        d_ref[s * blocks : (s + 1) * blocks, :] = all_ref[pl.ds(2 + s, blocks, stride=4), :]
    index = poles_ref[...]
    total = index.shape[0]
    bits = lambda size: size.bit_length() - 1
    s_of = index >> bits(half)
    device = (index & (half - 1)) >> bits(cols)
    lane_of = index & (cols - 1)
    chip_of = device >> bits(CORES)
    away = jnp.where(device & (CORES - 1) == core, 0, blocks // 2)
    row_of = s_of * blocks + away + chip_of
    rows = lax.broadcasted_iota(jnp.int32, (total, 2 * blocks), 1)
    pick = jnp.where(rows == row_of, 1.0, 0.0)
    picked = jnp.dot(pick, d_ref[...], precision=lax.Precision.HIGHEST, preferred_element_type=jnp.float32)
    lanes = lax.broadcasted_iota(jnp.int32, (total, cols), 1)
    value = jnp.sum(jnp.where(lanes == lane_of, picked, 0.0), axis=1, keepdims=True)
    pole_ref[...] = jnp.broadcast_to(value, (total, cols))
    roots = total // 2
    for t in range(roots // cols):
        low = to_lanes(pole_ref[t * cols : (t + 1) * cols, :])
        high = to_lanes(pole_ref[roots + t * cols : roots + (t + 1) * cols, :])
        bounds_ref[0:1, t * cols : (t + 1) * cols] = low
        bounds_ref[1:2, t * cols : (t + 1) * cols] = high - low
    own = roots // SHARE
    first = pl.multiple_of(slot * own, own)
    lower = pole_ref[pl.ds(first, own), :]
    spacing = pole_ref[pl.ds(roots + first, own), :] - lower
    inverse_coupling = 1.0 / jnp.full((own, cols), coupling_ref[0], jnp.float32)

    def sums(offset):
        def step(m, carry):
            total, slope = carry
            inverse = 1.0 / ((d_ref[pl.ds(m, 1), :] - lower) - offset)
            part = w_ref[pl.ds(m, 1), :] * inverse
            return total + part, slope + part * inverse

        zero = jnp.zeros((own, cols), jnp.float32)
        total, slope = lax.fori_loop(0, 2 * blocks, step, (zero, zero), unroll=4)
        spread = lambda a: jnp.broadcast_to(jnp.sum(a, axis=1, keepdims=True), (own, cols))
        return spread(total), spread(slope)

    def newton(_, offset):
        total, slope = sums(offset)
        moved = offset - (inverse_coupling + total) / slope
        return jnp.minimum(jnp.maximum(moved, 0.02 * spacing), 0.98 * spacing)

    offset = lax.fori_loop(0, ITERS, newton, 0.5 * spacing)
    _, norm_sq = sums(offset)
    row = lax.broadcasted_iota(jnp.int32, (own, cols), 0) + slot * own
    lane = lax.broadcasted_iota(jnp.int32, (own, cols), 1)
    for t in range(roots // cols):
        here = row == lane + t * cols
        for q, a in enumerate((offset, norm_sq)):
            roots_ref[q : q + 1, t * cols : (t + 1) * cols] = jnp.sum(jnp.where(here, a, 0.0), axis=0, keepdims=True)


def secular(same, other, poles, coupling, half):
    count, cols = same.shape
    roots = poles.shape[1]
    return pl.pallas_call(
        functools.partial(secular_kernel, half),
        in_specs=[VMEM(), VMEM(), VMEM(), SMEM()],
        out_specs=[VMEM(), VMEM()],
        out_shape=[jax.ShapeDtypeStruct((2, roots), jnp.float32)] * 2,
        scratch_shapes=[
            pltpu.VMEM((2 * count, cols), jnp.float32),
            pltpu.VMEM((count, cols), jnp.float32),
            pltpu.VMEM((count, cols), jnp.float32),
            pltpu.VMEM((2 * roots, cols), jnp.float32),
        ],
        compiler_params=params(8),
        cost_estimate=pl.CostEstimate(flops=20_000_000_000, bytes_accessed=400_000, transcendentals=0),
        name="secular",
    )(same, other, poles.reshape(-1, 1), coupling)


def vectors_kernel(chunks, chips, same_ref, other_ref, a_ref, b_ref, c_ref, e_ref, bounds_ref, mine_ref, theirs_ref,
                   high_ref, low_ref, position_ref, first_ref, mine_buf, theirs_buf, sems):
    copies = fetch(chunks, chips, mine_ref, theirs_ref, mine_buf, theirs_buf, sems)
    me = lax.axis_index("row")
    chip = me // CORES
    cols = same_ref.shape[1]
    found = (a_ref[...] + b_ref[...]) + (c_ref[...] + e_ref[...])
    offset, norm_sq = found[0:1, :], found[1:2, :]
    lower, spacing = bounds_ref[0:1, :], bounds_ref[1:2, :]
    position_ref[...] = offset / spacing
    normalizer = 1.0 / jnp.sqrt(norm_sq)
    roots = offset.shape[1]
    for p, ref in enumerate((same_ref, other_ref)):
        for s in range(2):
            z = jnp.broadcast_to(ref[pl.ds(chip * 4 + s, 1), :], (cols, cols)).T
            d = jnp.broadcast_to(ref[pl.ds(chip * 4 + 2 + s, 1), :], (cols, cols)).T
            for t in range(roots // cols):
                k = slice(t * cols, (t + 1) * cols)
                v = z / ((d - lower[:, k]) - offset[:, k]) * normalizer[:, k]
                high = v.astype(jnp.bfloat16)
                high_ref[s, p * cols : (p + 1) * cols, k] = high
                low_ref[s, p * cols : (p + 1) * cols, k] = (v - high.astype(jnp.float32)).astype(jnp.bfloat16)
    multiply(chunks, copies, mine_buf, theirs_buf, high_ref, low_ref, [first_ref])


def make_vectors(chunk, chips, same, other, found, bounds, mine, theirs):
    cols = same.shape[1]
    roots = bounds.shape[1]
    length = mine.shape[0] // chips // CORES
    return pl.pallas_call(
        functools.partial(vectors_kernel, [chunk], chips),
        in_specs=[VMEM()] * 7 + [ANY()] * 2,
        out_specs=[VMEM()] * 4,
        out_shape=[
            jax.ShapeDtypeStruct((2, CORES * cols, roots), jnp.bfloat16),
            jax.ShapeDtypeStruct((2, CORES * cols, roots), jnp.bfloat16),
            jax.ShapeDtypeStruct((1, roots), jnp.float32),
            jax.ShapeDtypeStruct((2, length // 2, roots), jnp.float32),
        ],
        scratch_shapes=[
            pltpu.VMEM((1, length, cols), jnp.float32),
            pltpu.VMEM((1, length, cols), jnp.float32),
            pltpu.SemaphoreType.DMA((1, 1, 2)),
        ],
        compiler_params=params(8),
        cost_estimate=pl.CostEstimate(flops=500_000_000, bytes_accessed=1_000_000, transcendentals=0),
        name="vectors",
    )(same, other, *found, bounds, mine, theirs)


def fetch(chunks, chips, own_ref, other_ref, own_buf, other_buf, sems):
    me = lax.axis_index("row")
    chip, core = me // CORES, lax.rem(me, CORES)
    length = own_ref.shape[0] // chips // CORES
    role = lax.rem(chip + core, CORES)
    copies = []
    for n, (distance, count, _) in enumerate(chunks):
        chunk = lax.rem(chip + jnp.where(role == 0, distance, chips - distance), chips)
        copies.append([])
        for h in range(count):
            start = pl.multiple_of(chunk * (CORES * length) + lax.rem(role + chunk + h, 2) * length, length)
            for q, (ref, buf) in enumerate(((own_ref, own_buf), (other_ref, other_buf))):
                copy = pltpu.make_async_copy(
                    ref.at[pl.ds(start, length), :], buf.at[n, pl.ds(h * length, length), :], sems.at[n, h, q]
                )
                copy.start()
                copies[n].append(copy)
    return copies


def multiply(chunks, copies, own_buf, other_buf, high_ref, low_ref, out_refs):
    most = max(count for _, count, _ in chunks)
    dot = functools.partial(jnp.dot, preferred_element_type=jnp.float32)
    outs = iter(out_refs)
    for n, (_, count, pieces) in enumerate(chunks):
        refs = [next(outs) for _ in pieces]
        rows = own_buf.shape[1] // most * count // 2
        for copy in copies[n]:
            copy.wait()

        @pl.loop(0, 2)
        def _(s):
            a = own_buf[n, pl.ds(s, rows, stride=2), :]
            b = other_buf[n, pl.ds(s, rows, stride=2), :]
            x = jnp.concatenate([a, b], axis=1)
            high = x.astype(jnp.bfloat16)
            low = (x - high.astype(jnp.float32)).astype(jnp.bfloat16)
            both = dot(jnp.concatenate([low, high], axis=0), high_ref[s])
            term = (both[:rows] + dot(high, low_ref[s])) + both[rows:]
            for ref, (first, last) in zip(refs, pieces):
                ref[s] = term[first:last]


def product_kernel(chunks, chips, own_ref, other_ref, high_ref, low_ref, *rest):
    *out_refs, own_buf, other_buf, sems = rest
    copies = fetch(chunks, chips, own_ref, other_ref, own_buf, other_buf, sems)
    multiply(chunks, copies, own_buf, other_buf, high_ref, low_ref, out_refs)


def product(chunks, chips, own, other, high, low):
    length = own.shape[0] // chips // CORES
    cols, roots = own.shape[1], high.shape[2]
    most = max(count for _, count, _ in chunks)
    work = sum(count for _, count, _ in chunks)
    pieces = [piece for _, _, some in chunks for piece in some]
    outs = pl.pallas_call(
        functools.partial(product_kernel, chunks, chips),
        in_specs=[ANY(), ANY(), VMEM(), VMEM()],
        out_specs=[VMEM()] * len(pieces),
        out_shape=[jax.ShapeDtypeStruct((2, last - first, roots), jnp.float32) for first, last in pieces],
        scratch_shapes=[
            pltpu.VMEM((len(chunks), most * length, cols), jnp.float32),
            pltpu.VMEM((len(chunks), most * length, cols), jnp.float32),
            pltpu.SemaphoreType.DMA((len(chunks), most, 2)),
        ],
        compiler_params=params(8),
        cost_estimate=pl.CostEstimate(flops=work * 300_000_000, bytes_accessed=work * 800_000, transcendentals=0),
        name=f"product{chunks[0][0]}",
    )(own, other, high, low)
    outs = iter(outs)
    return [[next(outs) for _ in some] for _, _, some in chunks]


def finish_kernel(a_ref, b_ref, c_ref, out_ref):
    for s in range(2):
        out_ref[:, s, :] = (a_ref[s] + b_ref[s]) + c_ref[s]


def finish(a, b, c):
    _, rows, roots = a.shape
    return pl.pallas_call(
        finish_kernel,
        in_specs=[VMEM()] * 3,
        out_specs=VMEM(),
        out_shape=jax.ShapeDtypeStruct((rows, 2, roots), jnp.float32),
        compiler_params=params(8),
        name="finish",
    )(a, b, c)


def body(sub_vectors, eigen_values, kept, poles, coupling):
    rows, _, cols = sub_vectors.shape
    n = lax.axis_size("row")
    chips = n // CORES
    swap = [(i, i ^ 1) for i in range(n)]
    neighbour = [(i, i ^ CORES) for i in range(n)]
    diagonal = [(i, i ^ (CORES + 1)) for i in range(n)]
    onward = []
    for i in range(n):
        chip, core = i // CORES, i % CORES
        there = (chip + (1, -1)[role_of(chip, core)]) % chips
        onward.append((i, there * CORES + (1 - core)))
    homeward = [(i, j ^ 1) for i, j in onward]
    send = functools.partial(lax.ppermute, axis_name="row")

    own = sub_vectors.reshape(rows * 2, cols)
    other = send(own, perm=swap)
    packed = pack(own, eigen_values, kept, chips)
    groups = [[i for i in range(n) if i % CORES == c] for c in range(CORES)]
    same = lax.all_to_all(packed, "row", 0, 0, tiled=True, axis_index_groups=groups).reshape(chips * 4, cols)
    across = send(same, perm=swap)
    roots, bounds = secular(same, across, poles, coupling, n * cols)
    found = [roots] + [send(roots, perm=p) for p in (neighbour, diagonal, swap)]

    half = rows // chips // CORES
    both = ((0, half), (half, 2 * half))
    far = chips // 2
    high, low, position, first = make_vectors((far, 1, both[:1]), chips, same, across, found, bounds, own, other)
    term = functools.partial(product, chips=chips, own=own, other=other, high=high, low=low)
    streams = [send(first, perm=onward), None]
    distance = far - 1
    while distance > 0:
        span = 1 if distance == far - 1 or distance == 1 else 2
        for terms in term([(d, 2, both) for d in range(distance, distance - span, -1)]):
            totals = [b if a is None else a + b for a, b in zip(streams, terms)]
            distance -= 1
            streams = [send(totals[0], perm=onward), send(totals[1], perm=onward if distance else homeward)]
    ((last,),) = term([(0, 1, both[:1])])
    merged = finish(streams[0], last, streams[1])
    return (position.reshape(-1), merged)


def solution(mesh):
    in_specs = (
        P("groups", None, "row"),
        P(None, ("groups", "row")),
        P(None, ("groups", "row")),
        P(None, "groups"),
        P("groups"),
    )
    out_specs = (P("groups"), P(("groups", "row"), None, None))
    return jax.shard_map(body, mesh=mesh, in_specs=in_specs, out_specs=out_specs, check_vma=False)
```
